512 devices in a mesh: dom: 128 (over z, x, core), tile: 4 (over y).
Axes of the slice: x: 4, y: 4, z: 16, core: 2. Of those that a mesh axis runs over, the one named last changes fastest.
Arguments:
- krylov_block: float32 [1536, 32, 128], P('dom'), may hold values from -6 to 6
- diag_block: float32 [1536, 128, 128], P(('dom', 'tile')), may hold values from -0.031819805 to 4.03182
- inverse_prev: float32 [1536, 128, 128], P(('dom', 'tile')), may hold values from -0.01767767 to 0.951011
- coupling_tiles: float32 [1536, 8, 128, 128], P('dom', 'tile'), may hold values from -0.14142136 to 0.14142136
- slot_kind: int32 [1536, 8], P('dom', 'tile'), may hold values from 0 to 2, as said below
- slot_link: int32 [1536, 8], P('dom', 'tile'), may hold values from 0 to 31, as said below
- send_slots: int32 [128, 4, 4, 4], P('dom', 'tile'), may hold values from 0 to 23, as said below
Outputs:
- inverse_new: float32 [1536, 128, 128], P(('dom', 'tile'))
- applied: float32 [1536, 32, 128], P('dom')
The draws below stay inside these ranges and needn't reach their ends.
Inputs may be any that keep to these rules, and one draw needn't show every extreme that they name: `slot_kind`: every live slot has exactly one partner as stated, in the same tile group and in a partition at most two away; partners never lie outside the partitions 0 .. 127. `slot_link`: links of empty slots are 0. `send_slots`: entry [p, g, l, j] is a slot position of partition p in group g. Lists 0 and 1 name upper slots whose partners lie in partition p + 1 and p + 2, lists 2 and 3 lower slots whose partners lie in p - 1 and p - 2; the four lists and the partition's own pairs use distinct positions. Some list reaches 4 live entries in every draw.
All inputs are finite; a program needn't handle non-finite values.
Results may differ from the reference program's by a relative error of at most 0.0003.
Values sent between devices are 32-bit elements; how exact they have to be, the bound alone decides.
A program may use at most 64 MiB of HBM per device.

```python
import jax
import jax.numpy as jnp
from jax import lax

BLK = 128
VECS = 32
RB = 12
KD = 2
FSWEEPS = 2
LSWEEPS = 3
USWEEPS = 3
NB = 1536
N_DOM = 128
N_TILE = 4


def slot_pattern(key):
    base = jax.random.fold_in(key, 7151)
    slot_total = RB * KD
    capacity = RB * KD // 5
    local_pairs = (slot_total - 4 * capacity) // 2
    device_keys = jax.random.split(jax.random.fold_in(base, 1), N_DOM * N_TILE)
    orders = jax.vmap(lambda item: jax.random.permutation(item, slot_total))(device_keys)
    orders = orders.reshape(N_DOM, N_TILE, slot_total).astype(jnp.int32)
    coins = jax.random.randint(jax.random.fold_in(base, 2), (2, N_DOM, N_TILE, capacity), 0, 10)
    salt = jax.random.randint(jax.random.fold_in(base, 3), (), 0, 4)
    domain_ids = jnp.arange(N_DOM, dtype=jnp.int32)[:, None, None]
    group_ids = jnp.arange(N_TILE, dtype=jnp.int32)[None, :, None]
    filled = (domain_ids + group_ids + salt) % 4 == 0
    reach = jnp.stack([domain_ids + 1 < N_DOM, domain_ids + 2 < N_DOM])
    live = ((coins < 7) | filled[None]) & reach
    lower_near = jnp.concatenate([jnp.zeros_like(live[0, :1]), live[0, :-1]], 0)
    lower_far = jnp.concatenate([jnp.zeros_like(live[1, :2]), live[1, :-2]], 0)
    kinds = jnp.zeros((N_DOM, N_TILE, slot_total), jnp.int32)
    links = jnp.zeros((N_DOM, N_TILE, slot_total), jnp.int32)
    domain_index = jnp.broadcast_to(domain_ids, (N_DOM, N_TILE, capacity))
    group_index = jnp.broadcast_to(group_ids, (N_DOM, N_TILE, capacity))
    offsets = jnp.arange(capacity, dtype=jnp.int32)[None, None, :]
    plan = ((0, 2, live[0], 0), (1, 2, live[1], capacity), (2, 1, lower_near, 0), (3, 1, lower_far, capacity))
    for list_no, side_code, active, shift_by in plan:
        places = orders[:, :, list_no * capacity:(list_no + 1) * capacity]
        kinds = kinds.at[domain_index, group_index, places].set(side_code * active.astype(jnp.int32))
        links = links.at[domain_index, group_index, places].set(jnp.where(active, slot_total + shift_by + offsets, 0))
    pair_coins = jax.random.randint(jax.random.fold_in(base, 4), (N_DOM, N_TILE, local_pairs), 0, 10) < 8
    start = 4 * capacity
    first = orders[:, :, start:start + 2 * local_pairs:2]
    second = orders[:, :, start + 1:start + 2 * local_pairs:2]
    usable = pair_coins & (first // KD != second // KD)
    lower_place = jnp.where(first // KD > second // KD, first, second)
    upper_place = jnp.where(first // KD > second // KD, second, first)
    pair_domain = jnp.broadcast_to(domain_ids, (N_DOM, N_TILE, local_pairs))
    pair_group = jnp.broadcast_to(group_ids, (N_DOM, N_TILE, local_pairs))
    kinds = kinds.at[pair_domain, pair_group, lower_place].set(jnp.where(usable, 1, 0))
    links = links.at[pair_domain, pair_group, lower_place].set(jnp.where(usable, upper_place, 0))
    kinds = kinds.at[pair_domain, pair_group, upper_place].set(jnp.where(usable, 2, 0))
    links = links.at[pair_domain, pair_group, upper_place].set(jnp.where(usable, lower_place, 0))
    sending = jnp.stack([orders[:, :, j * capacity:(j + 1) * capacity] for j in range(4)], 2)
    kind_out = kinds.reshape(N_DOM, N_TILE, RB, KD).transpose(0, 2, 1, 3).reshape(RB * N_DOM, N_TILE * KD)
    link_out = links.reshape(N_DOM, N_TILE, RB, KD).transpose(0, 2, 1, 3).reshape(RB * N_DOM, N_TILE * KD)
    return (kind_out.astype(jnp.int32), link_out.astype(jnp.int32), sending.astype(jnp.int32))


def pivot_pattern(key):
    base = jax.random.fold_in(key, 3301)
    row_total = RB * N_DOM
    pivot_gains = jnp.exp(jax.random.uniform(jax.random.fold_in(base, 1), (row_total, BLK), minval=jnp.log(1.5), maxval=jnp.log(4.0)))
    identity = jnp.eye(BLK, dtype=jnp.float32)
    jitter = 0.09 * BLK ** (-0.5) * jax.random.truncated_normal(jax.random.fold_in(base, 2), -4.0, 4.0, (row_total, BLK, BLK))
    diagonal = pivot_gains[:, :, None] * identity + jitter
    wobble = 1.0 + 0.2 * jax.random.truncated_normal(jax.random.fold_in(base, 3), -2.0, 2.0, (row_total, BLK))
    scatter_part = 0.05 * BLK ** (-0.5) * jax.random.truncated_normal(jax.random.fold_in(base, 4), -4.0, 4.0, (row_total, BLK, BLK))
    inverse = (wobble / pivot_gains)[:, :, None] * identity + scatter_part
    return (diagonal.astype(jnp.float32), inverse.astype(jnp.float32))


def draw_slot_kind(key, part):
    return slot_pattern(key)[0]


def draw_slot_link(key, part):
    return slot_pattern(key)[1]


def draw_send_slots(key, part):
    return slot_pattern(key)[2]


def draw_diag_block(key, part):
    return pivot_pattern(key)[0]


def draw_inverse_prev(key, part):
    return pivot_pattern(key)[1]


def steps_of(own_key, shape, cuts, least, largest):
    gain, own = 1.0, jax.random.fold_in(own_key, 6)
    for dim, shards_of in cuts:
        steps = jnp.exp(jax.random.uniform(jax.random.fold_in(own, dim), (shards_of,), jnp.float32, least / len(cuts), largest / len(cuts)))
        gain = gain * jnp.repeat(steps, shape[dim] // shards_of).reshape([-1 if axis == dim else 1 for axis in range(len(shape))])
    return gain


def noise(own_key, shape, scale, bound, cuts=(), held_as=jnp.bfloat16):
    entries = jax.random.normal(own_key, shape, jnp.float32) * scale
    if len(cuts) > 0:
        entries = steps_of(own_key, shape, cuts, -0.22, 0.18) * entries
    return jnp.clip(entries, min=-bound, max=bound).astype(held_as)


def setup_inputs(seed: int = 0) -> dict:
    seeds = jax.random.split(jax.random.key(seed), 8)
    return {
        "krylov_block": noise(seeds[0], (NB, VECS, BLK), 1.0, 6.0, ((0, 128),), jnp.float32),
        "diag_block": draw_diag_block(jax.random.fold_in(seeds[7], 71), 0),
        "inverse_prev": draw_inverse_prev(jax.random.fold_in(seeds[7], 71), 0),
        "coupling_tiles": noise(seeds[3], (NB, N_TILE * KD, BLK, BLK), (0.6 * BLK ** -0.5), 0.14142136, ((0, 128), (1, 4)), jnp.float32),
        "slot_kind": draw_slot_kind(jax.random.fold_in(seeds[7], 71), 0),
        "slot_link": draw_slot_link(jax.random.fold_in(seeds[7], 71), 0),
        "send_slots": draw_send_slots(jax.random.fold_in(seeds[7], 71), 0),
    }


precise = lax.Precision.HIGHEST


def newton_step(inverse, pivot):
    product = jnp.matmul(inverse, pivot, precision=precise)
    return 2.0 * inverse - jnp.matmul(product, inverse, precision=precise)


def apply_inverse(inverse, vectors):
    return jnp.einsum("rvj,rij->rvi", vectors, inverse, precision=precise)


def reference(krylov_block, diag_block, inverse_prev, coupling_tiles, slot_kind, slot_link, send_slots):
    block_size = coupling_tiles.shape[2]
    vector_count = krylov_block.shape[1]
    slot_total = RB * KD
    group_tiles = coupling_tiles.reshape(N_DOM, RB, N_TILE, KD, block_size, block_size)
    group_kind = slot_kind.reshape(N_DOM, RB, N_TILE, KD).transpose(0, 2, 1, 3).reshape(N_DOM, N_TILE, slot_total)
    group_link = slot_link.reshape(N_DOM, RB, N_TILE, KD).transpose(0, 2, 1, 3).reshape(N_DOM, N_TILE, slot_total)
    row_source = jnp.where(group_link < slot_total, group_link // KD, group_link - slot_total + RB).astype(jnp.int32)
    send_rows = (send_slots // KD).astype(jnp.int32)
    domains = jnp.arange(N_DOM, dtype=jnp.int32)
    diag_rows = diag_block.reshape(N_DOM, RB, block_size, block_size)

    def tiles_of(domain, side_code):
        local_tiles = group_tiles[domain].transpose(1, 0, 2, 3, 4).reshape(N_TILE, slot_total, block_size, block_size)
        return local_tiles * (group_kind[domain] == side_code).astype(jnp.float32)[:, :, None, None]

    def sent_products(inverse_rows, domain, which):
        source = jnp.clip(domain, 0, N_DOM - 1)
        valid = ((domain >= 0) & (domain < N_DOM)).astype(jnp.float32)
        upper_tiles = tiles_of(source, 2)
        picked_slots = send_slots[source, :, which].astype(jnp.int32)
        picked = jnp.take_along_axis(upper_tiles, picked_slots[:, :, None, None], axis=1)
        picked_inverse = inverse_rows[source][picked_slots // KD]
        return valid * jnp.einsum("tcij,tcjk->tcik", picked_inverse, picked, precision=precise)

    def pivots_of(inverse_rows):
        def one_domain(domain):
            repeated = jnp.repeat(inverse_rows[domain], KD, axis=0)
            products = jnp.einsum("cij,tcjk->tcik", repeated, tiles_of(domain, 2), precision=precise)
            near_part = sent_products(inverse_rows, domain - 1, 0)
            far_part = sent_products(inverse_rows, domain - 2, 1)
            lookup = jnp.concatenate([products, near_part, far_part], axis=1)
            gathered = jnp.take_along_axis(lookup, group_link[domain][:, :, None, None], axis=1)
            terms = jnp.einsum("tcij,tcjk->tcik", tiles_of(domain, 1), gathered, precision=precise)
            sums = terms.reshape(N_TILE, RB, KD, block_size, block_size).sum(axis=(0, 2))
            return diag_rows[domain] - sums
        return lax.map(one_domain, domains).reshape(RB * N_DOM, block_size, block_size)

    def neighbour_sum(values, side_code, direction, list_pair):
        grouped = values.reshape(N_DOM, RB, vector_count, block_size)

        def one_domain(domain):
            local_vals = grouped[domain]
            pieces = [jnp.broadcast_to(local_vals, (N_TILE,) + local_vals.shape)]
            for step_no, list_no in ((1, list_pair[0]), (2, list_pair[1])):
                target = domain - direction * step_no
                source = jnp.clip(target, 0, N_DOM - 1)
                valid = ((target >= 0) & (target < N_DOM)).astype(jnp.float32)
                pieces.append(valid * grouped[source][send_rows[source, :, list_no]])
            lookup = jnp.concatenate(pieces, axis=1)
            gathered = jnp.take_along_axis(lookup, row_source[domain][:, :, None, None], axis=1)
            terms = jnp.einsum("tcvj,tcij->tcvi", gathered, tiles_of(domain, side_code), precision=precise)
            return terms.reshape(N_TILE, RB, KD, vector_count, block_size).sum(axis=(0, 2))
        return lax.map(one_domain, domains).reshape(RB * N_DOM, vector_count, block_size)

    inverse = inverse_prev
    for sweep_no in range(FSWEEPS):
        pivots = pivots_of(inverse.reshape(N_DOM, RB, block_size, block_size))
        inverse = newton_step(inverse, pivots)
    lower_y = krylov_block
    for sweep_no in range(LSWEEPS):
        scaled = apply_inverse(inverse, lower_y)
        lower_y = krylov_block - neighbour_sum(scaled, 1, 1, (0, 1))
    solved = apply_inverse(inverse, lower_y)
    for sweep_no in range(USWEEPS):
        solved = apply_inverse(inverse, lower_y - neighbour_sum(solved, 2, -1, (2, 3)))
    return inverse, solved
```

```python
import jax
import jax.numpy as jnp
from jax import lax
from jax.experimental import pallas as pl
from jax.experimental.pallas import tpu as pltpu
from jax.sharding import PartitionSpec as P

FSWEEPS = 2
LSWEEPS = 3
USWEEPS = 3
MESH = pl.DeviceIdType.MESH
F32 = jnp.float32
BF16 = jnp.bfloat16
NN = (((1,), (0,)), ((), ()))
NT = (((1,), (1,)), ((), ()))


def split(x):
    hi = x.astype(BF16)
    lo = (x - hi.astype(F32)).astype(BF16)
    return hi, lo


def dot3(a, b, dims=NN):
    def one(p, q):
        return lax.dot_general(p, q, dims, preferred_element_type=F32)

    return one(a[0], b[0]) + (one(a[0], b[1]) + one(a[1], b[0]))


def make_kernel(n_dom, n_tile, rb, kd, blk, vecs, cap):
    own = rb // n_tile
    half = blk // 2
    slots = rb * kd
    sweeps = LSWEEPS + USWEEPS

    def kernel(
        kind, link, sends, kry, diag, inv, coup, inv_out, app_out,
        low_hi, low_lo, upp_hi, upp_lo, xall, out_q, part, fwd, pacc, ring_in, near_in2,
        vout, vpart, vrs, vfin, yown, send_sem, recv_sem, *tables,
    ):
        q_here, tables = tables[:FSWEEPS], tables[FSWEEPS:]
        q_there, tables = tables[:FSWEEPS], tables[FSWEEPS:]
        v_here, v_there = tables[:sweeps], tables[sweeps:]
        dom = lax.axis_index("dom")
        tile = lax.axis_index("tile")
        plus = {"tile": lax.rem(tile + 1, n_tile)}
        minus = {"tile": lax.rem(tile + n_tile - 1, n_tile)}
        doms = {d: {"dom": lax.rem(dom + n_dom + d, n_dom)} for d in (-2, -1, 1, 2)}

        barrier = pltpu.get_barrier_semaphore()
        peers = [{"tile": lax.rem(tile + d, n_tile)} for d in range(1, n_tile)]
        greeted = peers + list(doms.values())
        for dev in greeted:
            pl.semaphore_signal(barrier, inc=1, device_id=dev, device_id_type=MESH)
        pl.semaphore_wait(barrier, len(greeted))

        pending = []
        count = [0]

        def send(src, dst, dev):
            c = count[0]
            count[0] += 1
            copy = pltpu.make_async_remote_copy(
                src_ref=src, dst_ref=dst, send_sem=send_sem.at[c], recv_sem=recv_sem.at[c],
                device_id=dev, device_id_type=MESH,
            )
            copy.start()
            pending.append(copy)
            return copy

        def found(here, there, v, width):
            near = here[jnp.minimum(v, slots - 1) // width]
            remote = there[jnp.maximum(v - slots, 0)]
            return jnp.where(v < slots, near, remote)

        mine = pl.ds(tile * own, own)

        def gather_start(src, f):
            dst = xall.at[f]
            return (
                send(src.at[:, pl.ds(0, half)], dst.at[mine, pl.ds(0, half)], plus),
                send(src.at[:, pl.ds(half, half)], dst.at[mine, pl.ds(half, half)], minus),
                send(src.at[:, pl.ds(half, half)], dst.at[mine, pl.ds(half, half)], plus),
                send(src.at[:, pl.ds(0, half)], dst.at[mine, pl.ds(0, half)], minus),
            )

        def gather_finish(copies, f):
            dst = xall.at[f]
            left = pl.ds(lax.rem(tile + n_tile - 1, n_tile) * own, own)
            right = pl.ds(lax.rem(tile + 1, n_tile) * own, own)
            copies[0].wait_recv()
            a = dst.at[left, pl.ds(0, half)]
            more = send(a, a, plus)
            copies[1].wait_recv()
            b = dst.at[right, pl.ds(half, half)]
            more2 = send(b, b, minus)
            copies[2].wait_recv()
            copies[3].wait_recv()
            more.wait_recv()
            more2.wait_recv()

        first = gather_start(inv, 0)
        xall[0, mine] = inv[...]

        def prepare(r, _):
            for w in range(kd):
                cols = slice(w * blk, (w + 1) * blk)
                hi, lo = split(coup[r, w])
                zero = jnp.zeros_like(hi)
                k = kind[r, w]
                low_hi[r, :, cols] = jnp.where(k == 1, hi, zero)
                low_lo[r, :, cols] = jnp.where(k == 1, lo, zero)
                upp_hi[r, :, cols] = jnp.where(k == 2, hi, zero)
                upp_lo[r, :, cols] = jnp.where(k == 2, lo, zero)
            return _

        lax.fori_loop(0, rb, prepare, 0)
        gather_finish(first, 0)

        newest = inv
        for f in range(FSWEEPS):
            table, arrived = q_here[f], q_there[f]

            def upper(r, _):
                q = dot3(split(xall[f, r]), (upp_hi[r], upp_lo[r]))
                for w in range(kd):
                    table[r * kd + w] = q[:, w * blk : (w + 1) * blk]
                return _

            lax.fori_loop(0, rb, upper, 0, unroll=2)
            for l in range(2):
                for j in range(cap):
                    out_q[f, l * cap + j] = table[sends[l, j]]
            coming = [
                send(
                    out_q.at[f, pl.ds(l * cap, cap)],
                    arrived.at[pl.ds(l * cap, cap)],
                    doms[l + 1],
                )
                for l in range(2)
            ]
            for copy in coming:
                copy.wait_recv()

            def lower(r, _):
                q = jnp.concatenate([found(table, arrived, link[r, w], 1) for w in range(kd)], 0)
                part[f, r] = dot3((low_hi[r], low_lo[r]), split(q))
                return _

            lax.fori_loop(0, rb, lower, 0, unroll=2)

            far = pl.ds(lax.rem(tile + 2, n_tile) * own, own)
            right = pl.ds(lax.rem(tile + 1, n_tile) * own, own)
            left = pl.ds(lax.rem(tile + n_tile - 1, n_tile) * own, own)
            low_h, high_h = pl.ds(0, half), pl.ds(half, half)
            p = part.at[f]
            a = send(p.at[far, low_h], ring_in.at[f, 0], plus)
            b = send(p.at[far, high_h], ring_in.at[f, 1], minus)
            c = send(p.at[right, high_h], near_in2.at[f, 0, :, high_h], plus)
            d = send(p.at[left, low_h], near_in2.at[f, 1, :, low_h], minus)
            a.wait_recv()
            fwd[f, 0] = p[right, low_h] + ring_in[f, 0]
            e = send(fwd.at[f, 0], near_in2.at[f, 0, :, low_h], plus)
            b.wait_recv()
            fwd[f, 1] = p[left, high_h] + ring_in[f, 1]
            g = send(fwd.at[f, 1], near_in2.at[f, 1, :, high_h], minus)
            for copy in (c, d, e, g):
                copy.wait_recv()
            base = newest
            target = pacc.at[f]
            for i in range(own):
                pivot = diag[i] - (part[f, tile * own + i] + near_in2[f, 0, i] + near_in2[f, 1, i])
                x = base[i]
                xs = split(x)
                product = dot3(xs, split(pivot))
                target[i] = 2.0 * x - dot3(split(product), xs)
            newest = target
            if f < FSWEEPS - 1:
                copies = gather_start(target, f + 1)
                xall[f + 1, mine] = target[...]
                gather_finish(copies, f + 1)
        inv_out[...] = newest[...]

        def scaled(i, value):
            return dot3(split(value), split(newest[i]), NT)

        def spread_rows(dst):
            rows = dst.at[mine]
            copies = [send(rows, rows, peers[d]) for d in (1, 0, 2)]
            for copy in copies:
                copy.wait_recv()

        for i in range(own):
            v_here[0][tile * own + i] = scaled(i, kry[tile * own + i])
        for k in range(sweeps):
            lowering = k < LSWEEPS
            table, arrived = v_here[k], v_there[k]
            spread_rows(table)
            for l in range(2):
                for j in range(cap):
                    vout[k, l * cap + j] = table[sends[l + (0 if lowering else 2), j] // kd]
            sign = 1 if lowering else -1
            coming = [
                send(
                    vout.at[k, pl.ds(l * cap, cap)],
                    arrived.at[pl.ds(l * cap, cap)],
                    doms[sign * (l + 1)],
                )
                for l in range(2)
            ]
            for copy in coming:
                copy.wait_recv()
            hi_t, lo_t = (low_hi, low_lo) if lowering else (upp_hi, upp_lo)

            def products(r, _):
                v2 = jnp.concatenate([found(table, arrived, link[r, w], kd) for w in range(kd)], 1)
                vpart[k, r] = dot3(split(v2), (hi_t[r], lo_t[r]), NT)
                return _

            lax.fori_loop(0, rb, products, 0, unroll=3)
            copies = []
            for d in (1, 0, 2):
                rows = pl.ds(lax.rem(tile + d + 1, n_tile) * own, own)
                copies.append(send(vpart.at[k, rows], vrs.at[k, d], peers[d]))
            for copy in copies:
                copy.wait_recv()
            for i in range(own):
                total = vpart[k, tile * own + i] + vrs[k, 0, i] + vrs[k, 1, i] + vrs[k, 2, i]
                if lowering:
                    y = kry[tile * own + i] - total
                    if k == LSWEEPS - 1:
                        yown[i] = y
                    value = y
                else:
                    value = yown[i] - total
                result = scaled(i, value)
                if k < sweeps - 1:
                    v_here[k + 1][tile * own + i] = result
                else:
                    vfin[tile * own + i] = result
        spread_rows(vfin)
        app_out[...] = vfin[...]
        for copy in pending:
            copy.wait_send()

    return kernel


def solution(mesh):
    n_dom, n_tile = mesh.shape["dom"], mesh.shape["tile"]

    def local(krylov_block, diag_block, inverse_prev, coupling_tiles, slot_kind, slot_link, send_slots):
        rb, vecs, blk = krylov_block.shape
        kd = coupling_tiles.shape[1]
        cap = send_slots.shape[3]
        own = rb // n_tile
        slots = rb * kd
        sweeps = LSWEEPS + USWEEPS
        n_copies = FSWEEPS * (6 + 2 + 6) + sweeps * 8 + 3
        vm = pl.BlockSpec(memory_space=pltpu.VMEM)
        sm = pl.BlockSpec(memory_space=pltpu.SMEM)
        return pl.pallas_call(
            make_kernel(n_dom, n_tile, rb, kd, blk, vecs, cap),
            out_shape=(
                jax.ShapeDtypeStruct((own, blk, blk), F32),
                jax.ShapeDtypeStruct((rb, vecs, blk), F32),
            ),
            in_specs=[sm] * 3 + [vm] * 4,
            out_specs=(vm, vm),
            scratch_shapes=[
                pltpu.VMEM((rb, blk, kd * blk), BF16),
                pltpu.VMEM((rb, blk, kd * blk), BF16),
                pltpu.VMEM((rb, blk, kd * blk), BF16),
                pltpu.VMEM((rb, blk, kd * blk), BF16),
                pltpu.VMEM((FSWEEPS, rb, blk, blk), F32),
                pltpu.VMEM((FSWEEPS, 2 * cap, blk, blk), F32),
                pltpu.VMEM((FSWEEPS, rb, blk, blk), F32),
                pltpu.VMEM((FSWEEPS, 2, own, blk // 2, blk), F32),
                pltpu.VMEM((FSWEEPS, own, blk, blk), F32),
                pltpu.VMEM((FSWEEPS, 2, own, blk // 2, blk), F32),
                pltpu.VMEM((FSWEEPS, 2, own, blk, blk), F32),
                pltpu.VMEM((sweeps, 2 * cap, vecs, blk), F32),
                pltpu.VMEM((sweeps, rb, vecs, blk), F32),
                pltpu.VMEM((sweeps, n_tile - 1, own, vecs, blk), F32),
                pltpu.VMEM((rb, vecs, blk), F32),
                pltpu.VMEM((own, vecs, blk), F32),
                pltpu.SemaphoreType.DMA((n_copies,)),
                pltpu.SemaphoreType.DMA((n_copies,)),
            ]
            + [pltpu.VMEM((slots, blk, blk), F32)] * FSWEEPS
            + [pltpu.VMEM((2 * cap, blk, blk), F32)] * FSWEEPS
            + [pltpu.VMEM((rb, vecs, blk), F32)] * sweeps
            + [pltpu.VMEM((2 * cap, vecs, blk), F32)] * sweeps,
            compiler_params=pltpu.CompilerParams(
                collective_id=0, has_side_effects=True, vmem_limit_bytes=48 * 1024 * 1024
            ),
        )(
            slot_kind, slot_link, send_slots.reshape(4, cap),
            krylov_block, diag_block, inverse_prev, coupling_tiles,
        )

    placed = (
        P("dom", None, None),
        P(("dom", "tile"), None, None),
        P(("dom", "tile"), None, None),
        P("dom", "tile", None, None),
        P("dom", "tile"),
        P("dom", "tile"),
        P("dom", "tile", None, None),
    )
    return jax.shard_map(
        local,
        mesh=mesh,
        in_specs=placed,
        out_specs=(P(("dom", "tile"), None, None), P("dom", None, None)),
        check_vma=False,
    )
```

```python
import jax
import jax.numpy as jnp
from jax import lax
from jax.experimental import pallas as pl
from jax.experimental.pallas import tpu as pltpu
from jax.sharding import PartitionSpec as P

FSWEEPS = 2
LSWEEPS = 3
USWEEPS = 3
CHUNKS = 2
HALVES = 2
ROWS = 3
MESH = pl.DeviceIdType.MESH
F32 = jnp.float32
BF16 = jnp.bfloat16
NN = (((1,), (0,)), ((), ()))
NT = (((1,), (1,)), ((), ()))


def split(x):
    hi = x.astype(BF16)
    lo = (x - hi.astype(F32)).astype(BF16)
    return hi, lo


def dot3(a, b, dims=NN):
    def one(p, q):
        return lax.dot_general(p, q, dims, preferred_element_type=F32)

    return one(a[0], b[0]) + (one(a[0], b[1]) + one(a[1], b[0]))


def make_kernel(n_dom, n_tile, rb, kd, blk, vecs, cap):
    own = rb // n_tile
    slots = rb * kd
    sweeps = LSWEEPS + USWEEPS
    vc = vecs // CHUNKS
    part_rows = blk // HALVES
    piece = part_rows // 2
    half = blk // 2

    def kernel(
        kind_in, link_in, sends_in, kry_in, diag_in, inv_in, coup_in, inv_out, app_out,
        kind, link, sends, kry, diag, inv, coup, load_sem,
        low_hi, low_lo, upp_hi, upp_lo, xall, out_q, part, fwd, pacc, ring_in, near_in2, x_hi, x_lo,
        vout, vpart, vrs, vfin, yown, send_sem, recv_sem, *tables,
    ):
        q_here, tables = tables[:FSWEEPS], tables[FSWEEPS:]
        q_there, tables = tables[:FSWEEPS], tables[FSWEEPS:]
        v_here, v_there = tables[: sweeps * CHUNKS], tables[sweeps * CHUNKS :]

        sources = (inv_in, coup_in, sends_in, link_in, kind_in, diag_in, kry_in)
        targets = (inv, coup, sends, link, kind, diag, kry)
        loads = [
            pltpu.make_async_copy(a, b, load_sem.at[i]) for i, (a, b) in enumerate(zip(sources, targets))
        ]
        for load in loads:
            load.start()

        dom = lax.axis_index("dom")
        tile = lax.axis_index("tile")
        plus = {"tile": lax.rem(tile + 1, n_tile)}
        minus = {"tile": lax.rem(tile + n_tile - 1, n_tile)}
        doms = {d: {"dom": lax.rem(dom + n_dom + d, n_dom)} for d in (-2, -1, 1, 2)}

        barrier = pltpu.get_barrier_semaphore()
        peers = [{"tile": lax.rem(tile + d, n_tile)} for d in range(1, n_tile)]
        greeted = peers + list(doms.values())
        for dev in greeted:
            pl.semaphore_signal(barrier, inc=1, device_id=dev, device_id_type=MESH)
        loads[0].wait()
        pl.semaphore_wait(barrier, len(greeted))

        pending = []
        count = [0]

        def send(src, dst, dev):
            c = count[0]
            count[0] += 1
            copy = pltpu.make_async_remote_copy(
                src_ref=src, dst_ref=dst, send_sem=send_sem.at[c], recv_sem=recv_sem.at[c],
                device_id=dev, device_id_type=MESH,
            )
            copy.start()
            pending.append(copy)
            return copy

        def found(here, there, v, width, *rest):
            near = here[(jnp.minimum(v, slots - 1) // width, *rest)]
            remote = there[(jnp.maximum(v - slots, 0), *rest)]
            return jnp.where(v < slots, near, remote)

        def group(d):
            return lax.rem(tile + d, n_tile) * own

        mine, right, far, left = (pl.ds(group(d), own) for d in range(n_tile))

        class Gather:
            def __init__(self, src, f):
                self.src, self.dst, self.copies = src, xall.at[f], {}

            def cut(self, c, p):
                return pl.ds(c * part_rows + p * piece, piece)

            def out(self, c, p, dev):
                rows = self.cut(c, p)
                self.copies[c, p, dev is plus] = send(self.src.at[:, rows], self.dst.at[mine, rows], dev)

            def first(self, c):
                self.out(c, 0, plus)
                self.out(c, 1, minus)

            def second(self, c):
                self.out(c, 1, plus)
                self.out(c, 0, minus)

            def relay(self, c):
                for p, rows, dev in ((0, left, plus), (1, right, minus)):
                    self.copies[c, p, dev is plus].wait_recv()
                    block = self.dst.at[rows, self.cut(c, p)]
                    self.copies[c, p] = send(block, block, dev)

            def done(self, c):
                self.copies[c, 1, True].wait_recv()
                self.copies[c, 0, False].wait_recv()
                self.copies[c, 0].wait_recv()
                self.copies[c, 1].wait_recv()

        def prepare(r, _):
            for w in range(kd):
                cols = slice(w * blk, (w + 1) * blk)
                hi, lo = split(coup[r, w])
                zero = jnp.zeros_like(hi)
                k = kind[w, r]
                low_hi[r, :, cols] = jnp.where(k == 1, hi, zero)
                low_lo[r, :, cols] = jnp.where(k == 1, lo, zero)
                upp_hi[r, :, cols] = jnp.where(k == 2, hi, zero)
                upp_lo[r, :, cols] = jnp.where(k == 2, lo, zero)
            return _

        gather = Gather(inv, 0)
        for c in range(HALVES):
            gather.first(c)
            if c == 0:
                gather.second(c)
        xall[0, mine] = inv[...]

        newest = inv
        for f in range(FSWEEPS):
            table, arrived = q_here[f], q_there[f]
            gather.relay(0)
            for c in range(1, HALVES):
                gather.second(c)
            if f == 0:
                for load in loads[1:]:
                    load.wait()
                lax.fori_loop(0, rb, prepare, 0)
            coming = []
            for c in range(HALVES):
                gather.done(c)
                if c + 1 < HALVES:
                    gather.relay(c + 1)
                rows = pl.ds(c * part_rows, part_rows)

                def upper(r, _):
                    q = dot3(split(xall[f, r, rows]), (upp_hi[r], upp_lo[r]))
                    for w in range(kd):
                        table[r * kd + w, rows] = q[:, w * blk : (w + 1) * blk]
                    return _

                lax.fori_loop(0, rb, upper, 0, unroll=3)
                for l in (1, 0):
                    for j in range(cap):
                        out_q[f, l * cap + j, rows] = table[sends[l, j], rows]
                    cut = pl.ds(l * cap, cap)
                    coming.append(send(out_q.at[f, cut, rows], arrived.at[cut, rows], doms[l + 1]))
            for copy in coming:
                copy.wait_recv()

            def lower(base):
                for i in range(own):
                    r = base + i
                    q = jnp.concatenate([found(table, arrived, link[w, r], 1) for w in range(kd)], 0)
                    part[f, r] = dot3((low_hi[r], low_lo[r]), split(q))

            low_h, high_h = pl.ds(0, half), pl.ds(half, half)
            p = part.at[f]
            lower(group(2))
            a = send(p.at[far, low_h], ring_in.at[f, 0], plus)
            b = send(p.at[far, high_h], ring_in.at[f, 1], minus)
            lower(group(1))
            c = send(p.at[right, high_h], near_in2.at[f, 0, :, high_h], plus)
            lower(group(3))
            d = send(p.at[left, low_h], near_in2.at[f, 1, :, low_h], minus)
            a.wait_recv()
            fwd[f, 0] = p[right, low_h] + ring_in[f, 0]
            e = send(fwd.at[f, 0], near_in2.at[f, 0, :, low_h], plus)
            b.wait_recv()
            fwd[f, 1] = p[left, high_h] + ring_in[f, 1]
            g = send(fwd.at[f, 1], near_in2.at[f, 1, :, high_h], minus)
            lower(group(0))
            for copy in (c, d, e, g):
                copy.wait_recv()
            base = newest
            target = pacc.at[f]
            last = f == FSWEEPS - 1
            for i in range(own):
                pivot = diag[i] - (part[f, tile * own + i] + near_in2[f, 0, i] + near_in2[f, 1, i])
                x = base[i]
                xs = split(x)
                product = dot3(xs, split(pivot))
                fresh = 2.0 * x - dot3(split(product), xs)
                target[i] = fresh
                if last:
                    x_hi[i], x_lo[i] = split(fresh)
                else:
                    xall[f + 1, tile * own + i] = fresh
            newest = target
            if not last:
                gather = Gather(target, f + 1)
                for c in range(HALVES):
                    gather.first(c)
                    if c == 0:
                        gather.second(c)

        def scaled(i, value):
            return dot3(split(value), (x_hi[i], x_lo[i]), NT)

        def spread_rows(dst):
            rows = dst.at[mine]
            return [send(rows, rows, peers[d]) for d in (1, 0, 2)]

        def kry_rows(i, c):
            return kry[tile * own + i, c * vc : (c + 1) * vc]

        spreading = {}
        for c in range(CHUNKS):
            for i in range(own):
                v_here[c][tile * own + i] = scaled(i, kry_rows(i, c))
            spreading[c] = spread_rows(v_here[c])
        stores = [pltpu.make_async_copy(newest, inv_out, load_sem.at[0])]
        stores[0].start()
        for k in range(sweeps):
            lowering = k < LSWEEPS
            hi_t, lo_t = (low_hi, low_lo) if lowering else (upp_hi, upp_lo)
            sign = 1 if lowering else -1
            moving, summing = {}, {}
            for c in range(CHUNKS):
                table, arrived = v_here[k * CHUNKS + c], v_there[k * CHUNKS + c]
                for copy in spreading[c]:
                    copy.wait_recv()
                moving[c] = []
                for l in (1, 0):
                    for j in range(cap):
                        vout[k, c, l * cap + j] = table[sends[l + (0 if lowering else 2), j] // kd]
                    cut = pl.ds(l * cap, cap)
                    moving[c].append(send(vout.at[k, c, cut], arrived.at[cut], doms[sign * (l + 1)]))
            for c in range(CHUNKS):
                table, arrived = v_here[k * CHUNKS + c], v_there[k * CHUNKS + c]
                for copy in moving[c]:
                    copy.wait_recv()

                def products(r, _):
                    v2 = jnp.concatenate([found(table, arrived, link[w, r], kd) for w in range(kd)], 1)
                    vpart[k, c, r] = dot3(split(v2), (hi_t[r], lo_t[r]), NT)
                    return _

                lax.fori_loop(0, rb, products, 0, unroll=ROWS)
                summing[c] = []
                for d in (1, 0, 2):
                    rows = pl.ds(group(d + 1), own)
                    summing[c].append(send(vpart.at[k, c, rows], vrs.at[k, c, d], peers[d]))
            for c in range(CHUNKS):
                for copy in summing[c]:
                    copy.wait_recv()
                for i in range(own):
                    total = (
                        vpart[k, c, tile * own + i] + vrs[k, c, 0, i] + vrs[k, c, 1, i] + vrs[k, c, 2, i]
                    )
                    if lowering:
                        value = kry_rows(i, c) - total
                        if k == LSWEEPS - 1:
                            yown[c, i] = value
                    else:
                        value = yown[c, i] - total
                    result = scaled(i, value)
                    if k < sweeps - 1:
                        v_here[(k + 1) * CHUNKS + c][tile * own + i] = result
                    else:
                        vfin[c, tile * own + i] = result
                spreading[c] = spread_rows(v_here[(k + 1) * CHUNKS + c] if k < sweeps - 1 else vfin.at[c])
        for c in range(CHUNKS):
            for copy in spreading[c]:
                copy.wait_recv()
            stores.append(pltpu.make_async_copy(vfin.at[c], app_out.at[:, pl.ds(c * vc, vc)], load_sem.at[c + 1]))
            stores[-1].start()
        for copy in pending:
            copy.wait_send()
        for store in stores:
            store.wait()

    return kernel


def solution(mesh):
    n_dom, n_tile = mesh.shape["dom"], mesh.shape["tile"]

    def local(krylov_block, diag_block, inverse_prev, coupling_tiles, slot_kind, slot_link, send_slots):
        rb, vecs, blk = krylov_block.shape
        kd = coupling_tiles.shape[1]
        cap = send_slots.shape[3]
        own = rb // n_tile
        slots = rb * kd
        sweeps = LSWEEPS + USWEEPS
        vc = vecs // CHUNKS
        n_copies = FSWEEPS * (6 * HALVES + 2 * HALVES + 6) + CHUNKS * (sweeps * 8 + 3)
        hbm = pl.BlockSpec(memory_space=pltpu.HBM)
        return pl.pallas_call(
            make_kernel(n_dom, n_tile, rb, kd, blk, vecs, cap),
            out_shape=(
                jax.ShapeDtypeStruct((own, blk, blk), F32),
                jax.ShapeDtypeStruct((rb, vecs, blk), F32),
            ),
            in_specs=[hbm] * 7,
            out_specs=(hbm, hbm),
            scratch_shapes=[
                pltpu.SMEM((kd, rb), jnp.int32),
                pltpu.SMEM((kd, rb), jnp.int32),
                pltpu.SMEM((4, cap), jnp.int32),
                pltpu.VMEM((rb, vecs, blk), F32),
                pltpu.VMEM((own, blk, blk), F32),
                pltpu.VMEM((own, blk, blk), F32),
                pltpu.VMEM((rb, kd, blk, blk), F32),
                pltpu.SemaphoreType.DMA((7,)),
                pltpu.VMEM((rb, blk, kd * blk), BF16),
                pltpu.VMEM((rb, blk, kd * blk), BF16),
                pltpu.VMEM((rb, blk, kd * blk), BF16),
                pltpu.VMEM((rb, blk, kd * blk), BF16),
                pltpu.VMEM((FSWEEPS, rb, blk, blk), F32),
                pltpu.VMEM((FSWEEPS, 2 * cap, blk, blk), F32),
                pltpu.VMEM((FSWEEPS, rb, blk, blk), F32),
                pltpu.VMEM((FSWEEPS, 2, own, blk // 2, blk), F32),
                pltpu.VMEM((FSWEEPS, own, blk, blk), F32),
                pltpu.VMEM((FSWEEPS, 2, own, blk // 2, blk), F32),
                pltpu.VMEM((FSWEEPS, 2, own, blk, blk), F32),
                pltpu.VMEM((own, blk, blk), BF16),
                pltpu.VMEM((own, blk, blk), BF16),
                pltpu.VMEM((sweeps, CHUNKS, 2 * cap, vc, blk), F32),
                pltpu.VMEM((sweeps, CHUNKS, rb, vc, blk), F32),
                pltpu.VMEM((sweeps, CHUNKS, n_tile - 1, own, vc, blk), F32),
                pltpu.VMEM((CHUNKS, rb, vc, blk), F32),
                pltpu.VMEM((CHUNKS, own, vc, blk), F32),
                pltpu.SemaphoreType.DMA((n_copies,)),
                pltpu.SemaphoreType.DMA((n_copies,)),
            ]
            + [pltpu.VMEM((slots, blk, blk), F32)] * FSWEEPS
            + [pltpu.VMEM((2 * cap, blk, blk), F32)] * FSWEEPS
            + [pltpu.VMEM((rb, vc, blk), F32)] * (sweeps * CHUNKS)
            + [pltpu.VMEM((2 * cap, vc, blk), F32)] * (sweeps * CHUNKS),
            compiler_params=pltpu.CompilerParams(
                collective_id=0, has_side_effects=True, vmem_limit_bytes=66_600_000
            ),
        )(
            slot_kind.T, slot_link.T, send_slots.reshape(4, cap),
            krylov_block, diag_block, inverse_prev, coupling_tiles,
        )

    placed = (
        P("dom", None, None),
        P(("dom", "tile"), None, None),
        P(("dom", "tile"), None, None),
        P("dom", "tile", None, None),
        P("dom", "tile"),
        P("dom", "tile"),
        P("dom", "tile", None, None),
    )
    return jax.shard_map(
        local,
        mesh=mesh,
        in_specs=placed,
        out_specs=(P(("dom", "tile"), None, None), P("dom", None, None)),
        check_vma=False,
    )
```

```python
import jax
import jax.numpy as jnp
from jax import lax
from jax.experimental import pallas as pl
from jax.experimental.pallas import tpu as pltpu
from jax.sharding import PartitionSpec as P

FSWEEPS = 2
LSWEEPS = 3
USWEEPS = 3
CHUNKS = 2
HALVES = 2
ROWS = 3
MESH = pl.DeviceIdType.MESH
F32 = jnp.float32
BF16 = jnp.bfloat16
NN = (((1,), (0,)), ((), ()))
NT = (((1,), (1,)), ((), ()))


def split(x):
    hi = x.astype(BF16)
    lo = (x - hi.astype(F32)).astype(BF16)
    return hi, lo


def dot3(a, b, dims=NN):
    def one(p, q):
        return lax.dot_general(p, q, dims, preferred_element_type=F32)

    rows = a[0].shape[0]
    both = one(jnp.concatenate(a, 0), b[0])
    return both[:rows] + (one(a[0], b[1]) + both[rows:])


def make_kernel(n_dom, n_tile, rb, kd, blk, vecs, cap):
    own = rb // n_tile
    slots = rb * kd
    sweeps = LSWEEPS + USWEEPS
    vc = vecs // CHUNKS
    part_rows = blk // HALVES
    piece = part_rows // 2
    half = blk // 2

    def kernel(
        kind_in, link_in, sends_in, kry_in, diag_in, inv_in, coup_in, inv_out, app_out,
        kind, link, sends, kry, diag, inv, coup, load_sem,
        low_hi, low_lo, upp_hi, upp_lo, xall, out_q, part, fwd, pacc, ring_in, near_in2, x_hi, x_lo,
        vout, vpart, vrs, vfin, yown, send_sem, recv_sem, *tables,
    ):
        q_here, tables = tables[:FSWEEPS], tables[FSWEEPS:]
        q_there, tables = tables[:FSWEEPS], tables[FSWEEPS:]
        v_here, v_there = tables[: sweeps * CHUNKS], tables[sweeps * CHUNKS :]

        sources = (inv_in, coup_in, sends_in, link_in, kind_in, diag_in, kry_in)
        targets = (inv, coup, sends, link, kind, diag, kry)
        loads = [
            pltpu.make_async_copy(a, b, load_sem.at[i]) for i, (a, b) in enumerate(zip(sources, targets))
        ]
        for load in loads:
            load.start()

        dom = lax.axis_index("dom")
        tile = lax.axis_index("tile")
        plus = {"tile": lax.rem(tile + 1, n_tile)}
        minus = {"tile": lax.rem(tile + n_tile - 1, n_tile)}
        doms = {d: {"dom": lax.rem(dom + n_dom + d, n_dom)} for d in (-2, -1, 1, 2)}

        barrier = pltpu.get_barrier_semaphore()
        peers = [{"tile": lax.rem(tile + d, n_tile)} for d in range(1, n_tile)]
        greeted = peers + list(doms.values())
        for dev in greeted:
            pl.semaphore_signal(barrier, inc=1, device_id=dev, device_id_type=MESH)
        loads[0].wait()
        pl.semaphore_wait(barrier, len(greeted))

        pending = []
        count = [0]

        def send(src, dst, dev):
            c = count[0]
            count[0] += 1
            copy = pltpu.make_async_remote_copy(
                src_ref=src, dst_ref=dst, send_sem=send_sem.at[c], recv_sem=recv_sem.at[c],
                device_id=dev, device_id_type=MESH,
            )
            copy.start()
            pending.append(copy)
            return copy

        def found(here, there, v, width, *rest):
            near = here[(jnp.minimum(v, slots - 1) // width, *rest)]
            remote = there[(jnp.maximum(v - slots, 0), *rest)]
            return jnp.where(v < slots, near, remote)

        def group(d):
            return lax.rem(tile + d, n_tile) * own

        mine, right, far, left = (pl.ds(group(d), own) for d in range(n_tile))

        class Gather:
            def __init__(self, src, f):
                self.src, self.dst, self.copies = src, xall.at[f], {}

            def cut(self, c, p):
                return pl.ds(c * part_rows + p * piece, piece)

            def out(self, c, p, dev):
                rows = self.cut(c, p)
                self.copies[c, p, dev is plus] = send(self.src.at[:, rows], self.dst.at[mine, rows], dev)

            def lead(self, c):
                if 0 < c <= HALVES:
                    self.out(c - 1, 1, plus)
                    self.out(c - 1, 0, minus)
                if c < HALVES:
                    self.out(c, 0, plus)
                    self.out(c, 1, minus)

            def relay(self, c):
                for p, rows, dev in ((0, left, plus), (1, right, minus)):
                    self.copies[c, p, dev is plus].wait_recv()
                    block = self.dst.at[rows, self.cut(c, p)]
                    self.copies[c, p] = send(block, block, dev)
                self.lead(c + 2)

            def done(self, c):
                self.copies[c, 1, True].wait_recv()
                self.copies[c, 0, False].wait_recv()
                self.copies[c, 0].wait_recv()
                self.copies[c, 1].wait_recv()

        def prepare(r, _):
            for w in range(kd):
                cols = slice(w * blk, (w + 1) * blk)
                hi, lo = split(coup[r, w])
                zero = jnp.zeros_like(hi)
                k = kind[w, r]
                low_hi[r, :, cols] = jnp.where(k == 1, hi, zero)
                low_lo[r, :, cols] = jnp.where(k == 1, lo, zero)
                upp_hi[r, :, cols] = jnp.where(k == 2, hi, zero)
                upp_lo[r, :, cols] = jnp.where(k == 2, lo, zero)
            return _

        gather = Gather(inv, 0)
        gather.lead(0)
        gather.lead(1)
        xall[0, mine] = inv[...]

        newest = inv
        for f in range(FSWEEPS):
            table, arrived = q_here[f], q_there[f]
            gather.relay(0)
            if f == 0:
                for load in loads[1:]:
                    load.wait()
                lax.fori_loop(0, rb, prepare, 0)
            coming = []
            for c in range(HALVES):
                gather.done(c)
                if c + 1 < HALVES:
                    gather.relay(c + 1)
                rows = pl.ds(c * part_rows, part_rows)

                def upper(r, _):
                    q = dot3(split(xall[f, r, rows]), (upp_hi[r], upp_lo[r]))
                    for w in range(kd):
                        table[r * kd + w, rows] = q[:, w * blk : (w + 1) * blk]
                    return _

                lax.fori_loop(0, rb, upper, 0, unroll=3)
                for l in (1, 0):
                    for j in range(cap):
                        out_q[f, l * cap + j, rows] = table[sends[l, j], rows]
                    cut = pl.ds(l * cap, cap)
                    coming.append(send(out_q.at[f, cut, rows], arrived.at[cut, rows], doms[l + 1]))
            for copy in coming:
                copy.wait_recv()

            def lower(base):
                for i in range(own):
                    r = base + i
                    q = jnp.concatenate([found(table, arrived, link[w, r], 1) for w in range(kd)], 0)
                    part[f, r] = dot3((low_hi[r], low_lo[r]), split(q))

            low_h, high_h = pl.ds(0, half), pl.ds(half, half)
            p = part.at[f]
            lower(group(2))
            a = send(p.at[far, low_h], ring_in.at[f, 0], plus)
            b = send(p.at[far, high_h], ring_in.at[f, 1], minus)
            lower(group(1))
            c = send(p.at[right, high_h], near_in2.at[f, 0, :, high_h], plus)
            lower(group(3))
            d = send(p.at[left, low_h], near_in2.at[f, 1, :, low_h], minus)
            a.wait_recv()
            fwd[f, 0] = p[right, low_h] + ring_in[f, 0]
            e = send(fwd.at[f, 0], near_in2.at[f, 0, :, low_h], plus)
            b.wait_recv()
            fwd[f, 1] = p[left, high_h] + ring_in[f, 1]
            g = send(fwd.at[f, 1], near_in2.at[f, 1, :, high_h], minus)
            lower(group(0))
            for copy in (c, d, e, g):
                copy.wait_recv()
            base = newest
            target = pacc.at[f]
            last = f == FSWEEPS - 1
            pivots = []
            for i in range(own):
                pivot = diag[i] - (part[f, tile * own + i] + near_in2[f, 0, i] + near_in2[f, 1, i])
                pivots.append((split(pivot), split(base[i])))
            gather = None if last else Gather(target, f + 1)
            cuts = [pl.ds(0, blk)] if last else [pl.ds(0, half), pl.ds(half, half)]
            for h, rows in enumerate(cuts):
                for i in range(own):
                    x = base[i, rows]
                    product = dot3(split(x), pivots[i][0])
                    fresh = 2.0 * x - dot3(split(product), pivots[i][1])
                    target[i, rows] = fresh
                    if last:
                        x_hi[i], x_lo[i] = split(fresh)
                    else:
                        xall[f + 1, tile * own + i, rows] = fresh
                if not last:
                    gather.lead(h)
            newest = target

        def scaled(i, value):
            return dot3(split(value), (x_hi[i], x_lo[i]), NT)

        def spread_rows(dst):
            rows = dst.at[mine]
            return [send(rows, rows, peers[d]) for d in (1, 0, 2)]

        def kry_rows(i, c):
            return kry[tile * own + i, c * vc : (c + 1) * vc]

        spreading = {}
        for c in range(CHUNKS):
            for i in range(own):
                v_here[c][tile * own + i] = scaled(i, kry_rows(i, c))
            spreading[c] = spread_rows(v_here[c])
        inv_out[...] = newest[...]
        for k in range(sweeps):
            lowering = k < LSWEEPS
            hi_t, lo_t = (low_hi, low_lo) if lowering else (upp_hi, upp_lo)
            sign = 1 if lowering else -1
            moving, summing = {}, {}
            for c in range(CHUNKS):
                table, arrived = v_here[k * CHUNKS + c], v_there[k * CHUNKS + c]
                for copy in spreading[c]:
                    copy.wait_recv()
                moving[c] = []
                for l in (1, 0):
                    for j in range(cap):
                        vout[k, c, l * cap + j] = table[sends[l + (0 if lowering else 2), j] // kd]
                    cut = pl.ds(l * cap, cap)
                    moving[c].append(send(vout.at[k, c, cut], arrived.at[cut], doms[sign * (l + 1)]))
            for c in range(CHUNKS):
                table, arrived = v_here[k * CHUNKS + c], v_there[k * CHUNKS + c]
                for copy in moving[c]:
                    copy.wait_recv()

                def products(r, _):
                    v2 = jnp.concatenate([found(table, arrived, link[w, r], kd) for w in range(kd)], 1)
                    vpart[k, c, r] = dot3(split(v2), (hi_t[r], lo_t[r]), NT)
                    return _

                lax.fori_loop(0, rb, products, 0, unroll=ROWS)
                summing[c] = []
                for d in (1, 0, 2):
                    rows = pl.ds(group(d + 1), own)
                    summing[c].append(send(vpart.at[k, c, rows], vrs.at[k, c, d], peers[d]))
            for c in range(CHUNKS):
                for copy in summing[c]:
                    copy.wait_recv()
                for i in range(own):
                    total = (
                        vpart[k, c, tile * own + i] + vrs[k, c, 0, i] + vrs[k, c, 1, i] + vrs[k, c, 2, i]
                    )
                    if lowering:
                        value = kry_rows(i, c) - total
                        if k == LSWEEPS - 1:
                            yown[c, i] = value
                    else:
                        value = yown[c, i] - total
                    result = scaled(i, value)
                    if k < sweeps - 1:
                        v_here[(k + 1) * CHUNKS + c][tile * own + i] = result
                    else:
                        vfin[c, tile * own + i] = result
                spreading[c] = spread_rows(v_here[(k + 1) * CHUNKS + c] if k < sweeps - 1 else vfin.at[c])
        for c in range(CHUNKS):
            for copy in spreading[c]:
                copy.wait_recv()
            app_out[:, c * vc : (c + 1) * vc] = vfin[c]
        for copy in pending:
            copy.wait_send()

    return kernel


def solution(mesh):
    n_dom, n_tile = mesh.shape["dom"], mesh.shape["tile"]

    def local(krylov_block, diag_block, inverse_prev, coupling_tiles, slot_kind, slot_link, send_slots):
        rb, vecs, blk = krylov_block.shape
        kd = coupling_tiles.shape[1]
        cap = send_slots.shape[3]
        own = rb // n_tile
        slots = rb * kd
        sweeps = LSWEEPS + USWEEPS
        vc = vecs // CHUNKS
        n_copies = FSWEEPS * (6 * HALVES + 2 * HALVES + 6) + CHUNKS * (sweeps * 8 + 3)
        vm = pl.BlockSpec(memory_space=pltpu.VMEM)
        hbm = pl.BlockSpec(memory_space=pltpu.HBM)
        return pl.pallas_call(
            make_kernel(n_dom, n_tile, rb, kd, blk, vecs, cap),
            out_shape=(
                jax.ShapeDtypeStruct((own, blk, blk), F32),
                jax.ShapeDtypeStruct((rb, vecs, blk), F32),
            ),
            in_specs=[hbm] * 7,
            out_specs=(vm, vm),
            scratch_shapes=[
                pltpu.SMEM((kd, rb), jnp.int32),
                pltpu.SMEM((kd, rb), jnp.int32),
                pltpu.SMEM((4, cap), jnp.int32),
                pltpu.VMEM((rb, vecs, blk), F32),
                pltpu.VMEM((own, blk, blk), F32),
                pltpu.VMEM((own, blk, blk), F32),
                pltpu.VMEM((rb, kd, blk, blk), F32),
                pltpu.SemaphoreType.DMA((7,)),
                pltpu.VMEM((rb, blk, kd * blk), BF16),
                pltpu.VMEM((rb, blk, kd * blk), BF16),
                pltpu.VMEM((rb, blk, kd * blk), BF16),
                pltpu.VMEM((rb, blk, kd * blk), BF16),
                pltpu.VMEM((FSWEEPS, rb, blk, blk), F32),
                pltpu.VMEM((FSWEEPS, 2 * cap, blk, blk), F32),
                pltpu.VMEM((FSWEEPS, rb, blk, blk), F32),
                pltpu.VMEM((FSWEEPS, 2, own, blk // 2, blk), F32),
                pltpu.VMEM((FSWEEPS, own, blk, blk), F32),
                pltpu.VMEM((FSWEEPS, 2, own, blk // 2, blk), F32),
                pltpu.VMEM((FSWEEPS, 2, own, blk, blk), F32),
                pltpu.VMEM((own, blk, blk), BF16),
                pltpu.VMEM((own, blk, blk), BF16),
                pltpu.VMEM((sweeps, CHUNKS, 2 * cap, vc, blk), F32),
                pltpu.VMEM((sweeps, CHUNKS, rb, vc, blk), F32),
                pltpu.VMEM((sweeps, CHUNKS, n_tile - 1, own, vc, blk), F32),
                pltpu.VMEM((CHUNKS, rb, vc, blk), F32),
                pltpu.VMEM((CHUNKS, own, vc, blk), F32),
                pltpu.SemaphoreType.DMA((n_copies,)),
                pltpu.SemaphoreType.DMA((n_copies,)),
            ]
            + [pltpu.VMEM((slots, blk, blk), F32)] * FSWEEPS
            + [pltpu.VMEM((2 * cap, blk, blk), F32)] * FSWEEPS
            + [pltpu.VMEM((rb, vc, blk), F32)] * (sweeps * CHUNKS)
            + [pltpu.VMEM((2 * cap, vc, blk), F32)] * (sweeps * CHUNKS),
            compiler_params=pltpu.CompilerParams(
                collective_id=0, has_side_effects=True, vmem_limit_bytes=48 * 1024 * 1024
            ),
        )(
            *(
                pltpu.with_memory_space_constraint(x, pltpu.HBM)
                for x in (
                    slot_kind.T, slot_link.T, send_slots.reshape(4, cap),
                    krylov_block, diag_block, inverse_prev, coupling_tiles,
                )
            )
        )

    placed = (
        P("dom", None, None),
        P(("dom", "tile"), None, None),
        P(("dom", "tile"), None, None),
        P("dom", "tile", None, None),
        P("dom", "tile"),
        P("dom", "tile"),
        P("dom", "tile", None, None),
    )
    return jax.shard_map(
        local,
        mesh=mesh,
        in_specs=placed,
        out_specs=(P(("dom", "tile"), None, None), P("dom", None, None)),
        check_vma=False,
    )
```

```python
import jax
import jax.numpy as jnp
from jax import lax
from jax.experimental import pallas as pl
from jax.experimental.pallas import tpu as pltpu
from jax.sharding import PartitionSpec as P

FSWEEPS = 2
LSWEEPS = 3
USWEEPS = 3
CHUNKS = 4
HALVES = 2
ROWS = 12
MESH = pl.DeviceIdType.MESH
F32 = jnp.float32
BF16 = jnp.bfloat16
NN = (((1,), (0,)), ((), ()))
NT = (((1,), (1,)), ((), ()))


def split(x):
    hi = x.astype(BF16)
    lo = (x - hi.astype(F32)).astype(BF16)
    return hi, lo


def dot3(a, b, dims=NN):
    def one(p, q):
        return lax.dot_general(p, q, dims, preferred_element_type=F32)

    rows = a[0].shape[0]
    both = one(jnp.concatenate(a, 0), b[0])
    return both[:rows] + (one(a[0], b[1]) + both[rows:])


def make_kernel(n_dom, n_tile, rb, kd, blk, vecs, cap):
    own = rb // n_tile
    slots = rb * kd
    sweeps = LSWEEPS + USWEEPS
    vc = vecs // CHUNKS
    part_rows = blk // HALVES
    piece = part_rows // 2
    half = blk // 2

    def kernel(
        kind_in, link_in, sends_in, kry_in, diag_in, inv_in, coup_in, inv_out, app_out,
        kind, link, sends, kry, diag, inv, coup, load_sem,
        low_hi, low_lo, upp_hi, upp_lo, low_t_hi, low_t_lo, upp_t_hi, upp_t_lo, xall, out_q, part, fwd, pacc, ring_in, near_in2, x_hi, x_lo,
        vout, vpart, vrs, vfin, yown, send_sem, recv_sem, *tables,
    ):
        q_here, tables = tables[:FSWEEPS], tables[FSWEEPS:]
        q_there, tables = tables[:FSWEEPS], tables[FSWEEPS:]
        v_here, v_there = tables[: sweeps * CHUNKS], tables[sweeps * CHUNKS :]

        sources = (inv_in, coup_in, sends_in, link_in, kind_in, diag_in, kry_in)
        targets = (inv, coup, sends, link, kind, diag, kry)
        loads = [
            pltpu.make_async_copy(a, b, load_sem.at[i]) for i, (a, b) in enumerate(zip(sources, targets))
        ]
        for load in loads:
            load.start()

        dom = lax.axis_index("dom")
        tile = lax.axis_index("tile")
        plus = {"tile": lax.rem(tile + 1, n_tile)}
        minus = {"tile": lax.rem(tile + n_tile - 1, n_tile)}
        doms = {d: {"dom": lax.rem(dom + n_dom + d, n_dom)} for d in (-2, -1, 1, 2)}

        barrier = pltpu.get_barrier_semaphore()
        peers = [{"tile": lax.rem(tile + d, n_tile)} for d in range(1, n_tile)]
        greeted = peers + list(doms.values())
        for dev in greeted:
            pl.semaphore_signal(barrier, inc=1, device_id=dev, device_id_type=MESH)
        loads[0].wait()
        pl.semaphore_wait(barrier, len(greeted))

        pending = []
        count = [0]

        def send(src, dst, dev):
            c = count[0]
            count[0] += 1
            copy = pltpu.make_async_remote_copy(
                src_ref=src, dst_ref=dst, send_sem=send_sem.at[c], recv_sem=recv_sem.at[c],
                device_id=dev, device_id_type=MESH,
            )
            copy.start()
            pending.append(copy)
            return copy

        def found(here, there, v, width, *rest):
            near = here[(jnp.minimum(v, slots - 1) // width, *rest)]
            remote = there[(jnp.maximum(v - slots, 0), *rest)]
            return jnp.where(v < slots, near, remote)

        def group(d):
            return lax.rem(tile + d, n_tile) * own

        mine, right, far, left = (pl.ds(group(d), own) for d in range(n_tile))

        class Gather:
            def __init__(self, src, f):
                self.src, self.dst, self.copies = src, xall.at[f], {}

            def cut(self, c, p):
                return pl.ds(c * part_rows + p * piece, piece)

            def out(self, c, p, dev):
                rows = self.cut(c, p)
                self.copies[c, p, dev is plus] = send(self.src.at[:, rows], self.dst.at[mine, rows], dev)

            def lead(self, c):
                if 0 < c <= HALVES:
                    self.out(c - 1, 1, plus)
                    self.out(c - 1, 0, minus)
                if c < HALVES:
                    self.out(c, 0, plus)
                    self.out(c, 1, minus)

            def relay(self, c):
                for p, rows, dev in ((0, left, plus), (1, right, minus)):
                    self.copies[c, p, dev is plus].wait_recv()
                    block = self.dst.at[rows, self.cut(c, p)]
                    self.copies[c, p] = send(block, block, dev)
                self.lead(c + 2)

            def done(self, c):
                self.copies[c, 1, True].wait_recv()
                self.copies[c, 0, False].wait_recv()
                self.copies[c, 0].wait_recv()
                self.copies[c, 1].wait_recv()

        def prepare(r, _):
            for w in range(kd):
                cols = slice(w * blk, (w + 1) * blk)
                hi, lo = split(coup[r, w])
                zero = jnp.zeros_like(hi)
                k = kind[w, r]
                low_hi[r, :, cols] = jnp.where(k == 1, hi, zero)
                low_lo[r, :, cols] = jnp.where(k == 1, lo, zero)
                upp_hi[r, :, cols] = jnp.where(k == 2, hi, zero)
                upp_lo[r, :, cols] = jnp.where(k == 2, lo, zero)
            return _

        def flip(r, _):
            for w in range(kd):
                rows = slice(w * blk, (w + 1) * blk)
                hi, lo = split(coup[r, w].T)
                zero = jnp.zeros_like(hi)
                k = kind[w, r]
                low_t_hi[r, rows] = jnp.where(k == 1, hi, zero)
                low_t_lo[r, rows] = jnp.where(k == 1, lo, zero)
                upp_t_hi[r, rows] = jnp.where(k == 2, hi, zero)
                upp_t_lo[r, rows] = jnp.where(k == 2, lo, zero)
            return _

        gather = Gather(inv, 0)
        gather.lead(0)
        gather.lead(1)
        xall[0, mine] = inv[...]

        newest = inv
        for f in range(FSWEEPS):
            table, arrived = q_here[f], q_there[f]
            gather.relay(0)
            if f == 0:
                for load in loads[1:]:
                    load.wait()
                lax.fori_loop(0, rb, prepare, 0)
            coming = []
            for c in range(HALVES):
                gather.done(c)
                if c + 1 < HALVES:
                    gather.relay(c + 1)
                rows = pl.ds(c * part_rows, part_rows)

                def upper(r, _):
                    q = dot3(split(xall[f, r, rows]), (upp_hi[r], upp_lo[r]))
                    for w in range(kd):
                        table[r * kd + w, rows] = q[:, w * blk : (w + 1) * blk]
                    return _

                lax.fori_loop(0, rb, upper, 0, unroll=6)
                for l in (1, 0):
                    for j in range(cap):
                        out_q[f, l * cap + j, rows] = table[sends[l, j], rows]
                    cut = pl.ds(l * cap, cap)
                    coming.append(send(out_q.at[f, cut, rows], arrived.at[cut, rows], doms[l + 1]))
            if f == 0:
                lax.fori_loop(0, rb, flip, 0)
            for copy in coming:
                copy.wait_recv()

            def lower(base):
                for i in range(own):
                    r = base + i
                    q = jnp.concatenate([found(table, arrived, link[w, r], 1) for w in range(kd)], 0)
                    part[f, r] = dot3((low_hi[r], low_lo[r]), split(q))

            low_h, high_h = pl.ds(0, half), pl.ds(half, half)
            p = part.at[f]
            lower(group(2))
            a = send(p.at[far, low_h], ring_in.at[f, 0], plus)
            b = send(p.at[far, high_h], ring_in.at[f, 1], minus)
            lower(group(1))
            c = send(p.at[right, high_h], near_in2.at[f, 0, :, high_h], plus)
            lower(group(3))
            d = send(p.at[left, low_h], near_in2.at[f, 1, :, low_h], minus)
            a.wait_recv()
            fwd[f, 0] = p[right, low_h] + ring_in[f, 0]
            e = send(fwd.at[f, 0], near_in2.at[f, 0, :, low_h], plus)
            b.wait_recv()
            fwd[f, 1] = p[left, high_h] + ring_in[f, 1]
            g = send(fwd.at[f, 1], near_in2.at[f, 1, :, high_h], minus)
            lower(group(0))
            for copy in (c, d, e, g):
                copy.wait_recv()
            base = newest
            target = pacc.at[f]
            last = f == FSWEEPS - 1
            pivots = []
            for i in range(own):
                pivot = diag[i] - (part[f, tile * own + i] + near_in2[f, 0, i] + near_in2[f, 1, i])
                pivots.append((split(pivot), split(base[i])))
            gather = None if last else Gather(target, f + 1)
            cuts = [pl.ds(0, blk)] if last else [pl.ds(0, half), pl.ds(half, half)]
            for h, rows in enumerate(cuts):
                for i in range(own):
                    x = base[i, rows]
                    product = dot3(split(x), pivots[i][0])
                    fresh = 2.0 * x - dot3(split(product), pivots[i][1])
                    target[i, rows] = fresh
                    if last:
                        x_hi[i], x_lo[i] = split(fresh)
                    else:
                        xall[f + 1, tile * own + i, rows] = fresh
                if not last:
                    gather.lead(h)
            newest = target

        def scaled(i, value):
            return dot3(split(value), (x_hi[i], x_lo[i]), NT)

        def spread_rows(dst):
            rows = dst.at[mine]
            return [send(rows, rows, peers[d]) for d in (1, 0, 2)]

        def kry_rows(i, c):
            return kry[tile * own + i, c * vc : (c + 1) * vc]

        spreading = {}
        for c in range(CHUNKS):
            for i in range(own):
                v_here[c][tile * own + i] = scaled(i, kry_rows(i, c))
            spreading[c] = spread_rows(v_here[c])
        inv_out[...] = newest[...]
        for k in range(sweeps):
            lowering = k < LSWEEPS
            hi_t, lo_t = (low_t_hi, low_t_lo) if lowering else (upp_t_hi, upp_t_lo)
            sign = 1 if lowering else -1
            moving, summing = {}, {}
            for c in range(CHUNKS):
                table, arrived = v_here[k * CHUNKS + c], v_there[k * CHUNKS + c]
                for copy in spreading[c]:
                    copy.wait_recv()
                moving[c] = []
                for l in (1, 0):
                    for j in range(cap):
                        vout[k, c, l * cap + j] = table[sends[l + (0 if lowering else 2), j] // kd]
                    cut = pl.ds(l * cap, cap)
                    moving[c].append(send(vout.at[k, c, cut], arrived.at[cut], doms[sign * (l + 1)]))
            for c in range(CHUNKS):
                table, arrived = v_here[k * CHUNKS + c], v_there[k * CHUNKS + c]
                for copy in moving[c]:
                    copy.wait_recv()

                def products(r, _):
                    v2 = jnp.concatenate([found(table, arrived, link[w, r], kd) for w in range(kd)], 1)
                    vpart[k, c, r] = dot3(split(v2), (hi_t[r], lo_t[r]))
                    return _

                lax.fori_loop(0, rb, products, 0, unroll=ROWS)
                summing[c] = []
                for d in (1, 0, 2):
                    rows = pl.ds(group(d + 1), own)
                    summing[c].append(send(vpart.at[k, c, rows], vrs.at[k, c, d], peers[d]))
            for c in range(CHUNKS):
                for copy in summing[c]:
                    copy.wait_recv()
                for i in range(own):
                    total = (
                        vpart[k, c, tile * own + i] + vrs[k, c, 0, i] + vrs[k, c, 1, i] + vrs[k, c, 2, i]
                    )
                    if lowering:
                        value = kry_rows(i, c) - total
                        if k == LSWEEPS - 1:
                            yown[c, i] = value
                    else:
                        value = yown[c, i] - total
                    result = scaled(i, value)
                    if k < sweeps - 1:
                        v_here[(k + 1) * CHUNKS + c][tile * own + i] = result
                    else:
                        vfin[c, tile * own + i] = result
                spreading[c] = spread_rows(v_here[(k + 1) * CHUNKS + c] if k < sweeps - 1 else vfin.at[c])
        for c in range(CHUNKS):
            for copy in spreading[c]:
                copy.wait_recv()
            app_out[:, c * vc : (c + 1) * vc] = vfin[c]
        for copy in pending:
            copy.wait_send()

    return kernel


def solution(mesh):
    n_dom, n_tile = mesh.shape["dom"], mesh.shape["tile"]

    def local(krylov_block, diag_block, inverse_prev, coupling_tiles, slot_kind, slot_link, send_slots):
        rb, vecs, blk = krylov_block.shape
        kd = coupling_tiles.shape[1]
        cap = send_slots.shape[3]
        own = rb // n_tile
        slots = rb * kd
        sweeps = LSWEEPS + USWEEPS
        vc = vecs // CHUNKS
        n_copies = FSWEEPS * (6 * HALVES + 2 * HALVES + 6) + CHUNKS * (sweeps * 8 + 3)
        vm = pl.BlockSpec(memory_space=pltpu.VMEM)
        hbm = pl.BlockSpec(memory_space=pltpu.HBM)
        return pl.pallas_call(
            make_kernel(n_dom, n_tile, rb, kd, blk, vecs, cap),
            out_shape=(
                jax.ShapeDtypeStruct((own, blk, blk), F32),
                jax.ShapeDtypeStruct((rb, vecs, blk), F32),
            ),
            in_specs=[hbm] * 7,
            out_specs=(vm, vm),
            scratch_shapes=[
                pltpu.SMEM((kd, rb), jnp.int32),
                pltpu.SMEM((kd, rb), jnp.int32),
                pltpu.SMEM((4, cap), jnp.int32),
                pltpu.VMEM((rb, vecs, blk), F32),
                pltpu.VMEM((own, blk, blk), F32),
                pltpu.VMEM((own, blk, blk), F32),
                pltpu.VMEM((rb, kd, blk, blk), F32),
                pltpu.SemaphoreType.DMA((7,)),
                pltpu.VMEM((rb, blk, kd * blk), BF16),
                pltpu.VMEM((rb, blk, kd * blk), BF16),
                pltpu.VMEM((rb, blk, kd * blk), BF16),
                pltpu.VMEM((rb, blk, kd * blk), BF16),
                pltpu.VMEM((rb, kd * blk, blk), BF16),
                pltpu.VMEM((rb, kd * blk, blk), BF16),
                pltpu.VMEM((rb, kd * blk, blk), BF16),
                pltpu.VMEM((rb, kd * blk, blk), BF16),
                pltpu.VMEM((FSWEEPS, rb, blk, blk), F32),
                pltpu.VMEM((FSWEEPS, 2 * cap, blk, blk), F32),
                pltpu.VMEM((FSWEEPS, rb, blk, blk), F32),
                pltpu.VMEM((FSWEEPS, 2, own, blk // 2, blk), F32),
                pltpu.VMEM((FSWEEPS, own, blk, blk), F32),
                pltpu.VMEM((FSWEEPS, 2, own, blk // 2, blk), F32),
                pltpu.VMEM((FSWEEPS, 2, own, blk, blk), F32),
                pltpu.VMEM((own, blk, blk), BF16),
                pltpu.VMEM((own, blk, blk), BF16),
                pltpu.VMEM((sweeps, CHUNKS, 2 * cap, vc, blk), F32),
                pltpu.VMEM((sweeps, CHUNKS, rb, vc, blk), F32),
                pltpu.VMEM((sweeps, CHUNKS, n_tile - 1, own, vc, blk), F32),
                pltpu.VMEM((CHUNKS, rb, vc, blk), F32),
                pltpu.VMEM((CHUNKS, own, vc, blk), F32),
                pltpu.SemaphoreType.DMA((n_copies,)),
                pltpu.SemaphoreType.DMA((n_copies,)),
            ]
            + [pltpu.VMEM((slots, blk, blk), F32)] * FSWEEPS
            + [pltpu.VMEM((2 * cap, blk, blk), F32)] * FSWEEPS
            + [pltpu.VMEM((rb, vc, blk), F32)] * (sweeps * CHUNKS)
            + [pltpu.VMEM((2 * cap, vc, blk), F32)] * (sweeps * CHUNKS),
            compiler_params=pltpu.CompilerParams(
                collective_id=0, has_side_effects=True, vmem_limit_bytes=48 * 1024 * 1024
            ),
        )(
            *(
                pltpu.with_memory_space_constraint(x, pltpu.HBM)
                for x in (
                    slot_kind.T, slot_link.T, send_slots.reshape(4, cap),
                    krylov_block, diag_block, inverse_prev, coupling_tiles,
                )
            )
        )

    placed = (
        P("dom", None, None),
        P(("dom", "tile"), None, None),
        P(("dom", "tile"), None, None),
        P("dom", "tile", None, None),
        P("dom", "tile"),
        P("dom", "tile"),
        P("dom", "tile", None, None),
    )
    return jax.shard_map(
        local,
        mesh=mesh,
        in_specs=placed,
        out_specs=(P(("dom", "tile"), None, None), P("dom", None, None)),
        check_vma=False,
    )
```
